32 devices in a mesh: tm: 16 (over z, x, core), space: 2 (over y).
Axes of the slice: x: 2, y: 2, z: 4, core: 2. Of those that a mesh axis runs over, the one named last changes fastest.
Arguments:
- fine_nodes: float32 [16, 3, 3, 32, 4096], P('tm', None, None, 'space'), may hold values from -6 to 6
- init_state: float32 [3, 32, 4096], P(None, 'space'), may hold values from -6 to 6
- mean_depth: float32 [32, 4096], P('space'), may hold values from 0.5 to 2
Outputs:
- new_nodes: float32 [16, 3, 3, 32, 4096], P('tm', None, None, 'space')
The draws below stay inside these ranges and needn't reach their ends.
All inputs are finite; a program needn't handle non-finite values.
Results may differ from the reference program's by a relative error of at most 0.00002.
Values sent between devices are 32-bit elements; how exact they have to be, the bound alone decides.
A program may use at most 64 MiB of HBM per device.

```python
import math
import jax
import jax.numpy as jnp
from jax import lax

NX = 4096
NODES = 3
FIELDS = 3
NY = 32
SLICES = 16


def steps_of(rng, shape, pieces, least, largest):
    level, own = 1.0, jax.random.fold_in(rng, 6)
    for position, parts in pieces:
        heights = jnp.exp(jax.random.uniform(jax.random.fold_in(own, position), (parts,), jnp.float32, least / len(pieces), largest / len(pieces)))
        level = level * jnp.repeat(heights, shape[position] // parts).reshape([-1 if axis == position else 1 for axis in range(len(shape))])
    return level


def noise(key, extent, scale, limit, split=(), held_as=jnp.bfloat16):
    array = scale * jax.random.normal(key, extent, jnp.float32)
    if split:
        array = array * steps_of(key, extent, split, -0.22, 0.18)
    return jnp.clip(array, -limit, limit).astype(held_as)


def setup_inputs(seed: int = 0) -> dict:
    seeds = jax.random.split(jax.random.key(seed), 4)
    return {
        "fine_nodes": noise(seeds[0], (SLICES, NODES, FIELDS, NY, NX), 1.0, 6.0, ((0, 16), (3, 2)), jnp.float32),
        "init_state": noise(seeds[1], (FIELDS, NY, NX), 1.0, 6.0, ((1, 2),), jnp.float32),
        "mean_depth": jnp.clip(jnp.exp(math.log(2.0) - 1.3862944 * jax.random.uniform(seeds[2], (NY, NX), jnp.float32) ** steps_of(seeds[2], (NY, NX), ((0, 2),), -0.2, 0.2)), 0.5, 2.0),
    }


step_size = 0.3
viscosity = 1.0 / 3.0
coriolis = 0.5
quad_near = 5.0 / 24.0
quad_mid = 1.0 / 3.0
quad_far = -1.0 / 24.0


def column_slope(values):
    return (jnp.roll(values, -1, -1) - jnp.roll(values, 1, -1)) * 0.5


def row_slope(values):
    return (values[..., 2:, :] - values[..., :-2, :]) * 0.5


def diffuse(values, centre):
    return values[..., 2:, :] + values[..., :-2, :] + jnp.roll(centre, -1, -1) + jnp.roll(centre, 1, -1) - 4.0 * centre


def tendency(padded, depth_rows):
    height = padded[..., 0, :, :]
    east_flow = padded[..., 1, :, :]
    north_flow = padded[..., 2, :, :]
    centre = padded[..., 1:-1, :]
    height_c = centre[..., 0, :, :]
    east_c = centre[..., 1, :, :]
    north_c = centre[..., 2, :, :]
    depth_c = depth_rows[1:-1]
    height_rate = -column_slope(depth_c * east_c) - row_slope(depth_rows * north_flow) + viscosity * diffuse(height, height_c)
    east_rate = -column_slope(height_c) + coriolis * north_c + viscosity * diffuse(east_flow, east_c)
    north_rate = -row_slope(height) - coriolis * east_c + viscosity * diffuse(north_flow, north_c)
    return jnp.stack([height_rate, east_rate, north_rate], axis=-3)


def padded_rows(values):
    return jnp.concatenate([values[..., -1:, :], values, values[..., :1, :]], axis=-2)


def full_rate(values, mean_depth):
    return tendency(padded_rows(values), padded_rows(mean_depth))


def reference(fine_nodes, init_state, mean_depth):
    half_step = step_size * 0.5
    starts = jnp.concatenate([init_state[None], fine_nodes[:-1, 2]], axis=0)
    first_flags = jnp.arange(fine_nodes.shape[0], dtype=jnp.int32) == 0

    def slice_work(slice_items):
        points, section_zero, is_first = slice_items
        old_rates = full_rate(points, mean_depth)
        rate_zero = full_rate(section_zero, mean_depth)
        section_one = section_zero + half_step * (rate_zero - old_rates[0]) + step_size * (quad_near * old_rates[0] + quad_mid * old_rates[1] + quad_far * old_rates[2])
        rate_one = full_rate(section_one, mean_depth)
        section_two = section_one + half_step * (rate_one - old_rates[1]) + step_size * (quad_far * old_rates[0] + quad_mid * old_rates[1] + quad_near * old_rates[2])
        rate_two = full_rate(section_two, mean_depth)
        fas_term = -(step_size / 3.0) * (rate_zero - 2.0 * rate_one + rate_two)
        drift_total = half_step * (rate_two - rate_zero) + fas_term
        boosted = drift_total + jnp.where(is_first, section_zero + step_size * rate_zero, 0.0)
        return section_one, section_two, boosted

    section_ones, section_twos, boosts = lax.map(slice_work, (fine_nodes, starts, first_flags))

    def chain_turn(current, boosted):
        updated = boosted + (current + step_size * full_rate(current, mean_depth))
        return updated, updated

    _, coarse_end = lax.scan(chain_turn, jnp.zeros_like(init_state), boosts)
    coarse_begin = jnp.concatenate([init_state[None], coarse_end[:-1]], axis=0)
    middle = section_ones + 0.5 * ((coarse_begin - starts) + (coarse_end - section_twos))
    return jnp.stack([coarse_begin, middle, coarse_end], axis=1)
```

```python
import functools

import jax
import jax.numpy as jnp
from jax import lax
from jax.experimental import pallas as pl
from jax.experimental.pallas import tpu as pltpu
from jax.sharding import PartitionSpec as P

MESH = pl.DeviceIdType.MESH
DT = 0.3
NU = 1.0 / 3.0
FC = 0.5
LANES = 128
GROUPS = 4


def shift_left(v):
    return pltpu.roll(v, v.shape[1] - 1, 1)


def shift_right(v):
    return pltpu.roll(v, 1, 1)


def shift_up(v):
    return pltpu.roll(v, v.shape[0] - 1, 0)


def shift_down(v):
    return pltpu.roll(v, 1, 0)


def row_terms(h, e, n, depth):
    dn = 0.5 * (depth * n)
    nh, ne, nn, hh = NU * h, NU * e, NU * n, 0.5 * h
    return (nh - dn, ne, nn - hh), (nh + dn, ne, nn + hh)


def column_terms(h, e, n, depth):
    de = 0.5 * (depth * e)
    nh, ne, nn, hh = NU * h, NU * e, NU * n, 0.5 * h
    return (
        shift_left(nh - de) + shift_right(nh + de) - 4.0 * nh,
        shift_left(ne - hh) + shift_right(ne + hh) - 4.0 * ne + FC * n,
        shift_left(nn) + shift_right(nn) - 4.0 * nn - FC * e,
    )


def kernel(
    cfg, u_ref, init_ref, depth_ref, out_ref,
    s0, g, s1, mid, b, halo_src, dsrc, dep, main, halo, cs, ce, cb, esrc, edst,
    shift_s, shift_r, edge_s, edge_r, dep_s, dep_r, a2a_s, a2a_r, ret_s, ret_r, fwd_s, fwd_r,
):
    T, SP, RL, NX, W, K, stride, hw, per, nh = cfg
    p, y = lax.axis_index("tm"), lax.axis_index("space")
    me = p * SP + y
    total = T * SP
    mine = me // stride
    is_owner = lax.rem(me, stride) == 0

    def where(flat):
        return (flat // SP, lax.rem(flat, SP))

    barrier = pltpu.get_barrier_semaphore()

    @pl.loop(1, total)
    def _(i):
        pl.semaphore_signal(barrier, inc=1, device_id=where(lax.rem(me + i, total)), device_id_type=MESH)

    pl.semaphore_wait(barrier, total - 1)

    shift = pltpu.make_async_remote_copy(
        src_ref=u_ref.at[0, 2], dst_ref=s0, send_sem=shift_s, recv_sem=shift_r,
        device_id=(lax.rem(p + 1, T), y), device_id_type=MESH,
    )

    @pl.when(p < T - 1)
    def _():
        shift.start()

    lane_h = lax.broadcasted_iota(jnp.int32, (RL, LANES), 1)

    def dep_copy(yo):
        return pltpu.make_async_remote_copy(
            src_ref=dsrc.at[yo], dst_ref=dep.at[pl.ds(pl.multiple_of(y * RL, 8), RL)],
            send_sem=dep_s.at[yo], recv_sem=dep_r, device_id=(p, yo), device_id_type=MESH,
        )

    for yo in range(SP):
        flat = p * SP + yo
        k = flat // stride

        @pl.when(lax.rem(flat, stride) == 0)
        def _():
            here = depth_ref[:, pl.ds(pl.multiple_of(k * W, LANES), W)]
            after = depth_ref[:, pl.ds(pl.multiple_of(lax.rem((k + 1) * W, NX), LANES), LANES)]
            before = depth_ref[:, pl.ds(pl.multiple_of(lax.rem(k * W + NX - LANES, NX), LANES), LANES)]
            dsrc[yo, :, :W] = here
            dsrc[yo, :, W:] = jnp.where(lane_h < LANES // 2, after, before)

            @pl.when(yo != y)
            def _():
                dep_copy(yo).start()

            @pl.when(yo == y)
            def _():
                pltpu.make_async_copy(
                    dsrc.at[yo], dep.at[pl.ds(pl.multiple_of(y * RL, 8), RL)], dep_r
                ).start()

    for f in range(3):
        g[f] = (-7.0 / 24.0) * u_ref[0, 0, f] + (1.0 / 3.0) * u_ref[0, 1, f] - (1.0 / 24.0) * u_ref[0, 2, f]

    @pl.when(p > 0)
    def _():
        shift.wait_recv()

    @pl.when(p == 0)
    def _():
        s0[...] = init_ref[...]

    for f in range(3):
        g[f] = g[f] + 0.5 * s0[f]

    row = lax.broadcasted_iota(jnp.int32, (RL, NX), 0)

    def edge_copy(stage, side):
        to = lax.rem(y + SP - 1, SP) if side == 0 else lax.rem(y + 1, SP)
        return pltpu.make_async_remote_copy(
            src_ref=esrc.at[stage, side], dst_ref=edst.at[stage, side],
            send_sem=edge_s.at[stage, side], recv_sem=edge_r.at[stage, side],
            device_id=(p, to), device_id_type=MESH,
        )

    def rate_of_g(stage):
        up0, _ = row_terms(g[0, 0:1], g[1, 0:1], g[2, 0:1], depth_ref[0:1])
        _, down1 = row_terms(g[0, RL - 1 : RL], g[1, RL - 1 : RL], g[2, RL - 1 : RL], depth_ref[RL - 1 : RL])
        for f in range(3):
            esrc[stage, 0, f] = up0[f]
            esrc[stage, 1, f] = down1[f]
        for side in range(2):
            edge_copy(stage, side).start()
        h, e, n, depth = g[0], g[1], g[2], depth_ref[...]
        rates = column_terms(h, e, n, depth)
        ups, downs = row_terms(h, e, n, depth)
        for side in range(2):
            edge_copy(stage, side).wait_recv()
        return [
            rates[f]
            + jnp.where(row == RL - 1, edst[stage, 0, f], shift_up(ups[f]))
            + jnp.where(row == 0, edst[stage, 1, f], shift_down(downs[f]))
            for f in range(3)
        ]

    rates = rate_of_g(0)
    for f in range(3):
        s1[f] = s0[f] + DT * rates[f]
    for f in range(3):
        g[f] = (
            0.5 * s1[f]
            - (1.0 / 24.0) * u_ref[0, 0, f] - (1.0 / 6.0) * u_ref[0, 1, f] + (5.0 / 24.0) * u_ref[0, 2, f]
        )
    rates = rate_of_g(1)
    first = jnp.where(p == 0, 1.0, 0.0).astype(jnp.float32)
    for f in range(3):
        s2 = s1[f] + DT * rates[f]
        g[f] = (1.0 / 6.0) * s2 + (2.0 / 3.0) * s1[f] + (first - 5.0 / 6.0) * s0[f]
        mid[f] = s1[f] - 0.5 * (s0[f] + s2)
    rates = rate_of_g(2)
    for f in range(3):
        b[f] = first * s0[f] + DT * rates[f]

    slot_of = lax.rem(lane_h + hw, LANES) // (2 * hw)
    for k in range(K):
        lo, hi = ((k + 1) % K) * W, (k * W - LANES) % NX
        packed = [jnp.zeros((RL, LANES), jnp.float32) for _ in range(nh)]
        for f in range(3):
            z = jnp.where(lane_h < LANES // 2, b[f, :, lo : lo + LANES], b[f, :, hi : hi + LANES])
            slot = f % per
            if slot:
                z = pltpu.roll(z, 2 * hw * slot, 1)
            packed[f // per] = jnp.where(slot_of == slot, z, packed[f // per])
        for i in range(nh):
            halo_src[i, :, k * LANES : (k + 1) * LANES] = packed[i]

    my_rows = pl.ds(pl.multiple_of(y * RL, 8), RL)

    def a2a(k):
        ends = (
            (b.at[:, :, pl.ds(pl.multiple_of(k * W, LANES), W)], main.at[p, :, my_rows]),
            (halo_src.at[:, :, pl.ds(pl.multiple_of(k * LANES, LANES), LANES)], halo.at[p, :, my_rows]),
        )
        there = [
            pltpu.make_async_remote_copy(
                src_ref=src, dst_ref=dst, send_sem=a2a_s.at[i], recv_sem=a2a_r.at[i, p],
                device_id=where(k * stride), device_id_type=MESH,
            )
            for i, (src, dst) in enumerate(ends)
        ]
        here = [pltpu.make_async_copy(src, dst, a2a_r.at[i, p]) for i, (src, dst) in enumerate(ends)]
        return there, here

    @pl.loop(0, K)
    def _(i):
        k = lax.rem(mine + i, K)
        there, here = a2a(k)

        @pl.when(k * stride != me)
        def _():
            for copy in there:
                copy.start()

        @pl.when(k * stride == me)
        def _():
            for copy in here:
                copy.start()

    my_tile = pl.ds(pl.multiple_of(mine * W, LANES), W)
    my_group = mine // (K // GROUPS)

    def give_back(t):
        for yo in range(SP):
            src, dst = cs.at[t * SP + yo], ce.at[:, :, my_tile]
            here = jnp.logical_and(t == p, y == yo)

            @pl.when(jnp.logical_not(here))
            def _():
                pltpu.make_async_remote_copy(
                    src_ref=src, dst_ref=dst, send_sem=ret_s, recv_sem=ret_r.at[my_group],
                    device_id=(t, yo), device_id_type=MESH,
                ).start()

            @pl.when(here)
            def _():
                pltpu.make_async_copy(src, dst, ret_r.at[my_group]).start()

    def whole(ref, sem):
        pltpu.make_async_copy(ref, ref, sem).wait()

    @pl.when(is_owner)
    def _():
        whole(dep, dep_r)
        depth = dep[...]

        def turn(t, cur):
            h, e, n = cur
            rates = column_terms(h, e, n, depth)
            ups, downs = row_terms(h, e, n, depth)
            whole(main.at[t], a2a_r.at[0, t])
            whole(halo.at[t], a2a_r.at[1, t])
            new = []
            for f in range(3):
                tile = halo[t, f // per]
                if f % per:
                    tile = pltpu.roll(tile, LANES - 2 * hw * (f % per), 1)
                window = jnp.concatenate([main[t, f], tile], axis=1)
                value = window + cur[f] + DT * (rates[f] + shift_up(ups[f]) + shift_down(downs[f]))
                for yo in range(SP):
                    cs[t * SP + yo, f] = value[yo * RL : (yo + 1) * RL, :W]
                new.append(value)

            @pl.when(t > 0)
            def _():
                give_back(t - 1)

            return tuple(new)

        zero = jnp.zeros(dep.shape, jnp.float32)
        lax.fori_loop(0, T, turn, (zero, zero, zero))
        give_back(T - 1)

    width = NX // GROUPS

    def fwd(q):
        cols = pl.ds(q * width, width)
        return pltpu.make_async_remote_copy(
            src_ref=ce.at[:, :, cols], dst_ref=cb.at[:, :, cols],
            send_sem=fwd_s.at[q], recv_sem=fwd_r.at[q], device_id=(lax.rem(p + 1, T), y), device_id_type=MESH,
        )

    for q in range(GROUPS):
        whole(ce.at[:, :, pl.ds(q * width, width)], ret_r.at[q])

        @pl.when(p < T - 1)
        def _():
            fwd(q).start()

    @pl.when(p == 0)
    def _():
        cb[...] = init_ref[...]

    for q in range(GROUPS):
        @pl.when(p > 0)
        def _():
            fwd(q).wait_recv()

        cols = pl.ds(q * width, width)
        for f in range(3):
            start, end = cb[f, :, cols], ce[f, :, cols]
            out_ref[0, 0, f, :, cols] = start
            out_ref[0, 1, f, :, cols] = mid[f, :, cols] + 0.5 * (start + end)
            out_ref[0, 2, f, :, cols] = end

    @pl.when(p < T - 1)
    def _():
        shift.wait_send()
        for q in range(GROUPS):
            fwd(q).wait_send()

    for stage in range(3):
        for side in range(2):
            edge_copy(stage, side).wait_send()
    for yo in range(SP):
        flat = p * SP + yo

        @pl.when(jnp.logical_and(lax.rem(flat, stride) == 0, yo != y))
        def _():
            dep_copy(yo).wait_send()

    @pl.when(is_owner)
    def _():
        whole(b.at[:, :, pl.ds(0, (K - 1) * W)], a2a_s.at[0])
        whole(halo_src.at[:, :, pl.ds(0, (K - 1) * LANES)], a2a_s.at[1])
        whole(cs.at[pl.ds(0, total - 1)], ret_s)

    @pl.when(jnp.logical_not(is_owner))
    def _():
        whole(b, a2a_s.at[0])
        whole(halo_src, a2a_s.at[1])


def solution(mesh):
    T, SP = mesh.shape["tm"], mesh.shape["space"]

    def per_device(fine_nodes, init_state, mean_depth):
        RL, NX = mean_depth.shape
        total = T * SP
        W = max(LANES, NX // total)
        K = NX // W
        stride = total // K
        hw = 8
        while hw < T:
            hw *= 2
        per = LANES // (2 * hw)
        nh = -(-3 // per)
        cfg = (T, SP, RL, NX, W, K, stride, hw, per, nh)
        f32, dma = jnp.float32, pltpu.SemaphoreType.DMA
        state = pltpu.VMEM((3, RL, NX), f32)
        R = RL * SP
        vmem = pl.BlockSpec(memory_space=pltpu.VMEM)
        return pl.pallas_call(
            functools.partial(kernel, cfg),
            out_shape=jax.ShapeDtypeStruct(fine_nodes.shape, f32),
            in_specs=[vmem] * 3,
            out_specs=vmem,
            scratch_shapes=[
                state, state, state, state, state,
                pltpu.VMEM((nh, RL, K * LANES), f32),
                pltpu.VMEM((SP, RL, W + LANES), f32),
                pltpu.VMEM((R, W + LANES), f32),
                pltpu.VMEM((T, 3, R, W), f32),
                pltpu.VMEM((T, nh, R, LANES), f32),
                pltpu.VMEM((total, 3, RL, W), f32),
                state, state,
                pltpu.VMEM((3, 2, 3, 1, NX), f32),
                pltpu.VMEM((3, 2, 3, 1, NX), f32),
                dma, dma, dma((3, 2)), dma((3, 2)), dma((SP,)), dma, dma((2,)), dma((2, T)),
                dma, dma((GROUPS,)), dma((GROUPS,)), dma((GROUPS,)),
            ],
            compiler_params=pltpu.CompilerParams(
                collective_id=0, has_side_effects=True, vmem_limit_bytes=60 * 1024 * 1024
            ),
        )(fine_nodes, init_state, mean_depth)

    return jax.shard_map(
        per_device,
        mesh=mesh,
        in_specs=(P("tm", None, None, "space", None), P(None, "space", None), P("space", None)),
        out_specs=P("tm", None, None, "space", None),
        check_vma=False,
    )
```

```python
import functools

import jax
import jax.numpy as jnp
from jax import lax
from jax.experimental import pallas as pl
from jax.experimental.pallas import tpu as pltpu
from jax.sharding import PartitionSpec as P

MESH = pl.DeviceIdType.MESH
DT = 0.3
NU = 1.0 / 3.0
FC = 0.5
LANES = 128
GROUPS = 4


def shift_left(v):
    return pltpu.roll(v, v.shape[1] - 1, 1)


def shift_right(v):
    return pltpu.roll(v, 1, 1)


def shift_up(v):
    return pltpu.roll(v, v.shape[0] - 1, 0)


def shift_down(v):
    return pltpu.roll(v, 1, 0)


def row_terms(h, e, n, depth):
    dn = 0.5 * (depth * n)
    nh, ne, nn, hh = NU * h, NU * e, NU * n, 0.5 * h
    return (nh - dn, ne, nn - hh), (nh + dn, ne, nn + hh)


def column_terms(h, e, n, depth):
    de = 0.5 * (depth * e)
    nh, ne, nn, hh = NU * h, NU * e, NU * n, 0.5 * h
    return (
        shift_left(nh - de) + shift_right(nh + de) - 4.0 * nh,
        shift_left(ne - hh) + shift_right(ne + hh) - 4.0 * ne + FC * n,
        shift_left(nn) + shift_right(nn) - 4.0 * nn - FC * e,
    )


def kernel(
    cfg, u_ref, init_ref, depth_ref, out_ref,
    s0, g, s1, mid, b, halo_src, dsrc, dep, main, halo, cs, ce, cb, esrc, edst, cin, chalo, chalo_src,
    shift_s, shift_r, edge_s, edge_r, dep_s, dep_r, a2a_s, a2a_r, ret_s, ret_r, fwd_s, fwd_r,
    c_s, c_r, beg_s, beg_r,
):
    T, SP, RL, NX, W, K, stride, hw, per, nh, NG = cfg
    TG = T // NG
    p, y = lax.axis_index("tm"), lax.axis_index("space")
    me = p * SP + y
    total = T * SP
    block = p // TG
    pb = p - block * TG
    local = pb * SP + y
    mine = local // stride
    is_owner = lax.rem(local, stride) == 0
    even = lax.rem(p, 2) == 0

    def where(flat):
        return (flat // SP, lax.rem(flat, SP))

    barrier = pltpu.get_barrier_semaphore()

    @pl.loop(1, total)
    def _(i):
        pl.semaphore_signal(barrier, inc=1, device_id=where(lax.rem(me + i, total)), device_id_type=MESH)

    pl.semaphore_wait(barrier, total - 1)

    shift = pltpu.make_async_remote_copy(
        src_ref=u_ref.at[0, 2], dst_ref=s0, send_sem=shift_s, recv_sem=shift_r,
        device_id=(lax.rem(p + 1, T), y), device_id_type=MESH,
    )

    @pl.when(p < T - 1)
    def _():
        shift.start()

    lane_h = lax.broadcasted_iota(jnp.int32, (RL, LANES), 1)

    def dep_copy(yo):
        return pltpu.make_async_remote_copy(
            src_ref=dsrc.at[yo], dst_ref=dep.at[pl.ds(pl.multiple_of(y * RL, 8), RL)],
            send_sem=dep_s.at[yo], recv_sem=dep_r, device_id=(p, yo), device_id_type=MESH,
        )

    for yo in range(SP):
        flat = pb * SP + yo
        k = flat // stride

        @pl.when(lax.rem(flat, stride) == 0)
        def _():
            here = depth_ref[:, pl.ds(pl.multiple_of(k * W, LANES), W)]
            after = depth_ref[:, pl.ds(pl.multiple_of(lax.rem((k + 1) * W, NX), LANES), LANES)]
            before = depth_ref[:, pl.ds(pl.multiple_of(lax.rem(k * W + NX - LANES, NX), LANES), LANES)]
            dsrc[yo, :, :W] = here
            dsrc[yo, :, W:] = jnp.where(lane_h < LANES // 2, after, before)

            @pl.when(yo != y)
            def _():
                dep_copy(yo).start()

            @pl.when(yo == y)
            def _():
                pltpu.make_async_copy(
                    dsrc.at[yo], dep.at[pl.ds(pl.multiple_of(y * RL, 8), RL)], dep_r
                ).start()

    for f in range(3):
        g[f] = (-7.0 / 24.0) * u_ref[0, 0, f] + (1.0 / 3.0) * u_ref[0, 1, f] - (1.0 / 24.0) * u_ref[0, 2, f]

    @pl.when(p > 0)
    def _():
        shift.wait_recv()

    @pl.when(p == 0)
    def _():
        s0[...] = init_ref[...]

    for f in range(3):
        g[f] = g[f] + 0.5 * s0[f]

    row = lax.broadcasted_iota(jnp.int32, (RL, NX), 0)

    def edge_copy(stage, side):
        to = lax.rem(y + SP - 1, SP) if side == 0 else lax.rem(y + 1, SP)
        return pltpu.make_async_remote_copy(
            src_ref=esrc.at[stage, side], dst_ref=edst.at[stage, side],
            send_sem=edge_s.at[stage, side], recv_sem=edge_r.at[stage, side],
            device_id=(p, to), device_id_type=MESH,
        )

    def rate_of_g(stage):
        up0, _ = row_terms(g[0, 0:1], g[1, 0:1], g[2, 0:1], depth_ref[0:1])
        _, down1 = row_terms(g[0, RL - 1 : RL], g[1, RL - 1 : RL], g[2, RL - 1 : RL], depth_ref[RL - 1 : RL])
        for f in range(3):
            esrc[stage, 0, f] = up0[f]
            esrc[stage, 1, f] = down1[f]
        for side in range(2):
            edge_copy(stage, side).start()
        h, e, n, depth = g[0], g[1], g[2], depth_ref[...]
        rates = column_terms(h, e, n, depth)
        ups, downs = row_terms(h, e, n, depth)
        for side in range(2):
            edge_copy(stage, side).wait_recv()
        return [
            rates[f]
            + jnp.where(row == RL - 1, edst[stage, 0, f], shift_up(ups[f]))
            + jnp.where(row == 0, edst[stage, 1, f], shift_down(downs[f]))
            for f in range(3)
        ]

    rates = rate_of_g(0)
    for f in range(3):
        s1[f] = s0[f] + DT * rates[f]
    for f in range(3):
        g[f] = (
            0.5 * s1[f]
            - (1.0 / 24.0) * u_ref[0, 0, f] - (1.0 / 6.0) * u_ref[0, 1, f] + (5.0 / 24.0) * u_ref[0, 2, f]
        )
    rates = rate_of_g(1)
    first = jnp.where(p == 0, 1.0, 0.0).astype(jnp.float32)
    for f in range(3):
        s2 = s1[f] + DT * rates[f]
        g[f] = (1.0 / 6.0) * s2 + (2.0 / 3.0) * s1[f] + (first - 5.0 / 6.0) * s0[f]
        mid[f] = s1[f] - 0.5 * (s0[f] + s2)
    rates = rate_of_g(2)
    for f in range(3):
        b[f] = first * s0[f] + DT * rates[f]

    slot_of = lax.rem(lane_h + hw, LANES) // (2 * hw)
    for k in range(K):
        lo, hi = ((k + 1) % K) * W, (k * W - LANES) % NX
        packed = [jnp.zeros((RL, LANES), jnp.float32) for _ in range(nh)]
        for f in range(3):
            z = jnp.where(lane_h < LANES // 2, b[f, :, lo : lo + LANES], b[f, :, hi : hi + LANES])
            slot = f % per
            if slot:
                z = pltpu.roll(z, 2 * hw * slot, 1)
            packed[f // per] = jnp.where(slot_of == slot, z, packed[f // per])
        for i in range(nh):
            halo_src[i, :, k * LANES : (k + 1) * LANES] = packed[i]

    my_rows = pl.ds(pl.multiple_of(y * RL, 8), RL)

    def a2a(k):
        ends = (
            (b.at[:, :, pl.ds(pl.multiple_of(k * W, LANES), W)], main.at[pb, :, my_rows]),
            (halo_src.at[:, :, pl.ds(pl.multiple_of(k * LANES, LANES), LANES)], halo.at[pb, :, my_rows]),
        )
        there = [
            pltpu.make_async_remote_copy(
                src_ref=src, dst_ref=dst, send_sem=a2a_s.at[i], recv_sem=a2a_r.at[i, pb],
                device_id=where(block * TG * SP + k * stride), device_id_type=MESH,
            )
            for i, (src, dst) in enumerate(ends)
        ]
        here = [pltpu.make_async_copy(src, dst, a2a_r.at[i, pb]) for i, (src, dst) in enumerate(ends)]
        return there, here

    @pl.loop(0, K)
    def _(i):
        k = lax.rem(mine + i, K)
        there, here = a2a(k)

        @pl.when(k * stride != local)
        def _():
            for copy in there:
                copy.start()

        @pl.when(k * stride == local)
        def _():
            for copy in here:
                copy.start()

    my_tile = pl.ds(pl.multiple_of(mine * W, LANES), W)
    my_group = mine // (K // GROUPS)

    def give_back(t):
        for yo in range(SP):
            src, dst = cs.at[t * SP + yo], ce.at[:, :, my_tile]
            here = jnp.logical_and(t == pb, y == yo)

            @pl.when(jnp.logical_not(here))
            def _():
                pltpu.make_async_remote_copy(
                    src_ref=src, dst_ref=dst, send_sem=ret_s, recv_sem=ret_r.at[my_group],
                    device_id=(block * TG + t, yo), device_id_type=MESH,
                ).start()

            @pl.when(here)
            def _():
                pltpu.make_async_copy(src, dst, ret_r.at[my_group]).start()

    def give_begin(t, src):
        for yo in range(SP):
            dst = cb.at[:, :, my_tile]
            here = jnp.logical_and(t == pb, y == yo)

            @pl.when(jnp.logical_not(here))
            def _():
                pltpu.make_async_remote_copy(
                    src_ref=src.at[yo], dst_ref=dst, send_sem=beg_s.at[t * SP + yo], recv_sem=beg_r,
                    device_id=(block * TG + t, yo), device_id_type=MESH,
                ).start()

            @pl.when(here)
            def _():
                pltpu.make_async_copy(src.at[yo], dst, beg_r).start()

    def give(t):
        give_back(t)

        @pl.when(jnp.logical_and(lax.rem(t, 2) == 1, t < TG - 1))
        def _():
            give_begin(t + 1, cs.at[pl.ds(t * SP, SP)])

    def carry():
        ends = ((cs.at[pl.ds((TG - 1) * SP, SP)], cin), (chalo_src, chalo))
        return [
            pltpu.make_async_remote_copy(
                src_ref=src, dst_ref=dst, send_sem=c_s.at[i], recv_sem=c_r.at[i],
                device_id=(lax.rem(p + TG, T), y), device_id_type=MESH,
            )
            for i, (src, dst) in enumerate(ends)
        ]

    def unpack(tile, f):
        return pltpu.roll(tile, LANES - 2 * hw * (f % per), 1) if f % per else tile

    def whole(ref, sem):
        pltpu.make_async_copy(ref, ref, sem).wait()

    @pl.when(is_owner)
    def _():
        whole(dep, dep_r)
        depth = dep[...]

        def turn(t, cur):
            h, e, n = cur
            rates = column_terms(h, e, n, depth)
            ups, downs = row_terms(h, e, n, depth)
            whole(main.at[t], a2a_r.at[0, t])
            whole(halo.at[t], a2a_r.at[1, t])
            new = []
            for f in range(3):
                window = jnp.concatenate([main[t, f], unpack(halo[t, f // per], f)], axis=1)
                value = window + cur[f] + DT * (rates[f] + shift_up(ups[f]) + shift_down(downs[f]))
                for yo in range(SP):
                    cs[t * SP + yo, f] = value[yo * RL : (yo + 1) * RL, :W]
                new.append(value)

            @pl.when(jnp.logical_and(t > 0, block == NG - 1))
            def _():
                give(t - 1)

            return tuple(new)

        @pl.when(block == 0)
        def _():
            cin[...] = jnp.zeros_like(cin)
            chalo[...] = jnp.zeros_like(chalo)

        @pl.when(block > 0)
        def _():
            for copy in carry():
                copy.wait_recv()
            give_begin(0, cin)

        first_state = tuple(
            jnp.concatenate(
                [jnp.concatenate([cin[yo, f] for yo in range(SP)], axis=0), unpack(chalo[f // per], f)], axis=1
            )
            for f in range(3)
        )
        last = lax.fori_loop(0, TG, turn, first_state)

        @pl.when(block == NG - 1)
        def _():
            give(TG - 1)

        @pl.when(block < NG - 1)
        def _():
            lanes = lax.broadcasted_iota(jnp.int32, (SP * RL, LANES), 1)
            slots = lax.rem(lanes + hw, LANES) // (2 * hw)
            for i in range(nh):
                packed = jnp.zeros((SP * RL, LANES), jnp.float32)
                for f in range(i * per, min(3, (i + 1) * per)):
                    z = last[f][:, W:]
                    if f % per:
                        z = pltpu.roll(z, 2 * hw * (f % per), 1)
                    packed = jnp.where(slots == f % per, z, packed)
                chalo_src[i] = packed
            for copy in carry():
                copy.start()

            @pl.loop(0, TG)
            def _(t):
                give(t)

    width = NX // GROUPS

    def fwd(q):
        cols = pl.ds(q * width, width)
        return pltpu.make_async_remote_copy(
            src_ref=ce.at[:, :, cols], dst_ref=cb.at[:, :, cols],
            send_sem=fwd_s.at[q], recv_sem=fwd_r.at[q], device_id=(lax.rem(p + 1, T), y), device_id_type=MESH,
        )

    for q in range(GROUPS):
        whole(ce.at[:, :, pl.ds(q * width, width)], ret_r.at[q])

        @pl.when(even)
        def _():
            fwd(q).start()

    @pl.when(p == 0)
    def _():
        cb[...] = init_ref[...]

    @pl.when(jnp.logical_and(even, p > 0))
    def _():
        whole(cb, beg_r)

    for q in range(GROUPS):
        @pl.when(jnp.logical_not(even))
        def _():
            fwd(q).wait_recv()

        cols = pl.ds(q * width, width)
        for f in range(3):
            start, end = cb[f, :, cols], ce[f, :, cols]
            out_ref[0, 0, f, :, cols] = start
            out_ref[0, 1, f, :, cols] = mid[f, :, cols] + 0.5 * (start + end)
            out_ref[0, 2, f, :, cols] = end

    @pl.when(p < T - 1)
    def _():
        shift.wait_send()

    @pl.when(even)
    def _():
        for q in range(GROUPS):
            fwd(q).wait_send()

    for stage in range(3):
        for side in range(2):
            edge_copy(stage, side).wait_send()
    for yo in range(SP):
        flat = pb * SP + yo

        @pl.when(jnp.logical_and(lax.rem(flat, stride) == 0, yo != y))
        def _():
            dep_copy(yo).wait_send()

    @pl.when(is_owner)
    def _():
        whole(b.at[:, :, pl.ds(0, (K - 1) * W)], a2a_s.at[0])
        whole(halo_src.at[:, :, pl.ds(0, (K - 1) * LANES)], a2a_s.at[1])
        whole(cs.at[pl.ds(0, TG * SP - 1)], ret_s)

        @pl.when(block < NG - 1)
        def _():
            for copy in carry():
                copy.wait_send()

        for t in range(0, TG, 2):
            for yo in range(SP):
                sent = jnp.logical_not(jnp.logical_and(t == pb, y == yo))
                if t == 0:
                    sent = jnp.logical_and(sent, block > 0)

                @pl.when(sent)
                def _():
                    pltpu.make_async_copy(cin.at[yo], cin.at[yo], beg_s.at[t * SP + yo]).wait()

    @pl.when(jnp.logical_not(is_owner))
    def _():
        whole(b, a2a_s.at[0])
        whole(halo_src, a2a_s.at[1])


def solution(mesh):
    T, SP = mesh.shape["tm"], mesh.shape["space"]

    def per_device(fine_nodes, init_state, mean_depth):
        RL, NX = mean_depth.shape
        NG = 2 if T % 4 == 0 else 1
        members = T // NG * SP
        W = max(LANES, NX // members)
        K = NX // W
        stride = members // K
        hw = 8
        while hw < T:
            hw *= 2
        per = LANES // (2 * hw)
        nh = -(-3 // per)
        cfg = (T, SP, RL, NX, W, K, stride, hw, per, nh, NG)
        f32, dma = jnp.float32, pltpu.SemaphoreType.DMA
        state = pltpu.VMEM((3, RL, NX), f32)
        R = RL * SP
        vmem = pl.BlockSpec(memory_space=pltpu.VMEM)
        return pl.pallas_call(
            functools.partial(kernel, cfg),
            out_shape=jax.ShapeDtypeStruct(fine_nodes.shape, f32),
            in_specs=[vmem] * 3,
            out_specs=vmem,
            scratch_shapes=[
                state, state, state, state, state,
                pltpu.VMEM((nh, RL, K * LANES), f32),
                pltpu.VMEM((SP, RL, W + LANES), f32),
                pltpu.VMEM((R, W + LANES), f32),
                pltpu.VMEM((T // NG, 3, R, W), f32),
                pltpu.VMEM((T // NG, nh, R, LANES), f32),
                pltpu.VMEM((members, 3, RL, W), f32),
                state, state,
                pltpu.VMEM((3, 2, 3, 1, NX), f32),
                pltpu.VMEM((3, 2, 3, 1, NX), f32),
                pltpu.VMEM((SP, 3, RL, W), f32),
                pltpu.VMEM((nh, R, LANES), f32),
                pltpu.VMEM((nh, R, LANES), f32),
                dma, dma, dma((3, 2)), dma((3, 2)), dma((SP,)), dma, dma((2,)), dma((2, T // NG)),
                dma, dma((GROUPS,)), dma((GROUPS,)), dma((GROUPS,)),
                dma((2,)), dma((2,)), dma((members,)), dma,
            ],
            compiler_params=pltpu.CompilerParams(
                collective_id=0, has_side_effects=True, vmem_limit_bytes=60 * 1024 * 1024
            ),
        )(fine_nodes, init_state, mean_depth)

    return jax.shard_map(
        per_device,
        mesh=mesh,
        in_specs=(P("tm", None, None, "space", None), P(None, "space", None), P("space", None)),
        out_specs=P("tm", None, None, "space", None),
        check_vma=False,
    )
```

```python
import functools

import jax
import jax.numpy as jnp
from jax import lax
from jax.experimental import pallas as pl
from jax.experimental.pallas import tpu as pltpu
from jax.sharding import PartitionSpec as P

MESH = pl.DeviceIdType.MESH
DT = 0.3
NU = 1.0 / 3.0
FC = 0.5
LANES = 128
GROUPS = 4


def shift_left(v):
    return pltpu.roll(v, v.shape[1] - 1, 1)


def shift_right(v):
    return pltpu.roll(v, 1, 1)


def shift_up(v):
    return pltpu.roll(v, v.shape[0] - 1, 0)


def shift_down(v):
    return pltpu.roll(v, 1, 0)


def row_terms(h, e, n, depth):
    dn = 0.5 * (depth * n)
    nh, ne, nn, hh = NU * h, NU * e, NU * n, 0.5 * h
    return (nh - dn, ne, nn - hh), (nh + dn, ne, nn + hh)


def column_terms(h, e, n, depth):
    de = 0.5 * (depth * e)
    nh, ne, nn, hh = NU * h, NU * e, NU * n, 0.5 * h
    return (
        shift_left(nh - de) + shift_right(nh + de) - 4.0 * nh,
        shift_left(ne - hh) + shift_right(ne + hh) - 4.0 * ne + FC * n,
        shift_left(nn) + shift_right(nn) - 4.0 * nn - FC * e,
    )


def kernel(
    cfg, u_hbm, init_hbm, depth_hbm, out_ref, u_ref, init_ref, depth_ref,
    s0, g, s1, mid, b, halo_src, dsrc, dep, main, halo, cs, ce, cb, esrc, edst, cin, chalo, chalo_src,
    shift_s, shift_r, edge_s, edge_r, dep_s, dep_r, a2a_s, a2a_r, ret_s, ret_r, fwd_s, fwd_r,
    c_s, c_r, beg_s, beg_r, in_s,
):
    T, SP, RL, NX, W, K, stride, hw, per, nh, NG = cfg
    TG = T // NG
    p, y = lax.axis_index("tm"), lax.axis_index("space")
    me = p * SP + y
    total = T * SP
    block = p // TG
    pb = p - block * TG
    local = pb * SP + y
    mine = local // stride
    is_owner = lax.rem(local, stride) == 0
    even = lax.rem(p, 2) == 0

    def where(flat):
        return (flat // SP, lax.rem(flat, SP))

    barrier = pltpu.get_barrier_semaphore()

    @pl.loop(1, total)
    def _(i):
        pl.semaphore_signal(barrier, inc=1, device_id=where(lax.rem(me + i, total)), device_id_type=MESH)

    loads = [pltpu.make_async_copy(u_hbm.at[0, i], u_ref.at[i], in_s.at[i]) for i in (2, 0, 1)]
    loads.append(pltpu.make_async_copy(depth_hbm, depth_ref, in_s.at[3]))
    loads.append(pltpu.make_async_copy(init_hbm, init_ref, in_s.at[4]))
    for copy in loads:
        copy.start()
    loads[0].wait()
    pl.semaphore_wait(barrier, total - 1)

    shift = pltpu.make_async_remote_copy(
        src_ref=u_ref.at[2], dst_ref=s0, send_sem=shift_s, recv_sem=shift_r,
        device_id=(lax.rem(p + 1, T), y), device_id_type=MESH,
    )

    @pl.when(p < T - 1)
    def _():
        shift.start()

    for copy in loads[1:]:
        copy.wait()

    lane_h = lax.broadcasted_iota(jnp.int32, (RL, LANES), 1)

    def dep_copy(yo):
        return pltpu.make_async_remote_copy(
            src_ref=dsrc.at[yo], dst_ref=dep.at[pl.ds(pl.multiple_of(y * RL, 8), RL)],
            send_sem=dep_s.at[yo], recv_sem=dep_r, device_id=(p, yo), device_id_type=MESH,
        )

    for yo in range(SP):
        flat = pb * SP + yo
        k = flat // stride

        @pl.when(lax.rem(flat, stride) == 0)
        def _():
            here = depth_ref[:, pl.ds(pl.multiple_of(k * W, LANES), W)]
            after = depth_ref[:, pl.ds(pl.multiple_of(lax.rem((k + 1) * W, NX), LANES), LANES)]
            before = depth_ref[:, pl.ds(pl.multiple_of(lax.rem(k * W + NX - LANES, NX), LANES), LANES)]
            dsrc[yo, :, :W] = here
            dsrc[yo, :, W:] = jnp.where(lane_h < LANES // 2, after, before)

            @pl.when(yo != y)
            def _():
                dep_copy(yo).start()

            @pl.when(yo == y)
            def _():
                pltpu.make_async_copy(
                    dsrc.at[yo], dep.at[pl.ds(pl.multiple_of(y * RL, 8), RL)], dep_r
                ).start()

    for f in range(3):
        g[f] = (-7.0 / 24.0) * u_ref[0, f] + (1.0 / 3.0) * u_ref[1, f] - (1.0 / 24.0) * u_ref[2, f]

    @pl.when(p > 0)
    def _():
        shift.wait_recv()

    @pl.when(p == 0)
    def _():
        s0[...] = init_ref[...]

    for f in range(3):
        g[f] = g[f] + 0.5 * s0[f]

    row = lax.broadcasted_iota(jnp.int32, (RL, NX), 0)

    def edge_copy(stage, side):
        to = lax.rem(y + SP - 1, SP) if side == 0 else lax.rem(y + 1, SP)
        return pltpu.make_async_remote_copy(
            src_ref=esrc.at[stage, side], dst_ref=edst.at[stage, side],
            send_sem=edge_s.at[stage, side], recv_sem=edge_r.at[stage, side],
            device_id=(p, to), device_id_type=MESH,
        )

    def rate_of_g(stage):
        up0, _ = row_terms(g[0, 0:1], g[1, 0:1], g[2, 0:1], depth_ref[0:1])
        _, down1 = row_terms(g[0, RL - 1 : RL], g[1, RL - 1 : RL], g[2, RL - 1 : RL], depth_ref[RL - 1 : RL])
        for f in range(3):
            esrc[stage, 0, f] = up0[f]
            esrc[stage, 1, f] = down1[f]
        for side in range(2):
            edge_copy(stage, side).start()
        h, e, n, depth = g[0], g[1], g[2], depth_ref[...]
        rates = column_terms(h, e, n, depth)
        ups, downs = row_terms(h, e, n, depth)
        for side in range(2):
            edge_copy(stage, side).wait_recv()
        return [
            rates[f]
            + jnp.where(row == RL - 1, edst[stage, 0, f], shift_up(ups[f]))
            + jnp.where(row == 0, edst[stage, 1, f], shift_down(downs[f]))
            for f in range(3)
        ]

    rates = rate_of_g(0)
    for f in range(3):
        s1[f] = s0[f] + DT * rates[f]
    for f in range(3):
        g[f] = (
            0.5 * s1[f]
            - (1.0 / 24.0) * u_ref[0, f] - (1.0 / 6.0) * u_ref[1, f] + (5.0 / 24.0) * u_ref[2, f]
        )
    rates = rate_of_g(1)
    first = jnp.where(p == 0, 1.0, 0.0).astype(jnp.float32)
    for f in range(3):
        s2 = s1[f] + DT * rates[f]
        g[f] = (1.0 / 6.0) * s2 + (2.0 / 3.0) * s1[f] + (first - 5.0 / 6.0) * s0[f]
        mid[f] = s1[f] - 0.5 * (s0[f] + s2)
    rates = rate_of_g(2)
    for f in range(3):
        b[f] = first * s0[f] + DT * rates[f]

    slot_of = lax.rem(lane_h + hw, LANES) // (2 * hw)
    for k in range(K):
        lo, hi = ((k + 1) % K) * W, (k * W - LANES) % NX
        packed = [jnp.zeros((RL, LANES), jnp.float32) for _ in range(nh)]
        for f in range(3):
            z = jnp.where(lane_h < LANES // 2, b[f, :, lo : lo + LANES], b[f, :, hi : hi + LANES])
            slot = f % per
            if slot:
                z = pltpu.roll(z, 2 * hw * slot, 1)
            packed[f // per] = jnp.where(slot_of == slot, z, packed[f // per])
        for i in range(nh):
            halo_src[i, :, k * LANES : (k + 1) * LANES] = packed[i]

    my_rows = pl.ds(pl.multiple_of(y * RL, 8), RL)

    def a2a(k):
        ends = (
            (b.at[:, :, pl.ds(pl.multiple_of(k * W, LANES), W)], main.at[pb, :, my_rows]),
            (halo_src.at[:, :, pl.ds(pl.multiple_of(k * LANES, LANES), LANES)], halo.at[pb, :, my_rows]),
        )
        there = [
            pltpu.make_async_remote_copy(
                src_ref=src, dst_ref=dst, send_sem=a2a_s.at[i], recv_sem=a2a_r.at[i, pb],
                device_id=where(block * TG * SP + k * stride), device_id_type=MESH,
            )
            for i, (src, dst) in enumerate(ends)
        ]
        here = [pltpu.make_async_copy(src, dst, a2a_r.at[i, pb]) for i, (src, dst) in enumerate(ends)]
        return there, here

    @pl.loop(0, K)
    def _(i):
        k = lax.rem(mine + i, K)
        there, here = a2a(k)

        @pl.when(k * stride != local)
        def _():
            for copy in there:
                copy.start()

        @pl.when(k * stride == local)
        def _():
            for copy in here:
                copy.start()

    my_tile = pl.ds(pl.multiple_of(mine * W, LANES), W)
    my_group = mine // (K // GROUPS)

    def give_back(t):
        for yo in range(SP):
            src, dst = cs.at[t * SP + yo], ce.at[:, :, my_tile]
            here = jnp.logical_and(t == pb, y == yo)

            @pl.when(jnp.logical_not(here))
            def _():
                pltpu.make_async_remote_copy(
                    src_ref=src, dst_ref=dst, send_sem=ret_s, recv_sem=ret_r.at[my_group],
                    device_id=(block * TG + t, yo), device_id_type=MESH,
                ).start()

            @pl.when(here)
            def _():
                pltpu.make_async_copy(src, dst, ret_r.at[my_group]).start()

    def give_begin(t, src):
        for yo in range(SP):
            dst = cb.at[:, :, my_tile]
            here = jnp.logical_and(t == pb, y == yo)

            @pl.when(jnp.logical_not(here))
            def _():
                pltpu.make_async_remote_copy(
                    src_ref=src.at[yo], dst_ref=dst, send_sem=beg_s.at[t * SP + yo], recv_sem=beg_r,
                    device_id=(block * TG + t, yo), device_id_type=MESH,
                ).start()

            @pl.when(here)
            def _():
                pltpu.make_async_copy(src.at[yo], dst, beg_r).start()

    def give(t):
        give_back(t)

        @pl.when(jnp.logical_and(lax.rem(t, 2) == 1, t < TG - 1))
        def _():
            give_begin(t + 1, cs.at[pl.ds(t * SP, SP)])

    def carry():
        ends = ((cs.at[pl.ds((TG - 1) * SP, SP)], cin), (chalo_src, chalo))
        return [
            pltpu.make_async_remote_copy(
                src_ref=src, dst_ref=dst, send_sem=c_s.at[i], recv_sem=c_r.at[i],
                device_id=(lax.rem(p + TG, T), y), device_id_type=MESH,
            )
            for i, (src, dst) in enumerate(ends)
        ]

    def unpack(tile, f):
        return pltpu.roll(tile, LANES - 2 * hw * (f % per), 1) if f % per else tile

    def whole(ref, sem):
        pltpu.make_async_copy(ref, ref, sem).wait()

    @pl.when(is_owner)
    def _():
        whole(dep, dep_r)
        depth = dep[...]

        def turn(t, cur):
            h, e, n = cur
            rates = column_terms(h, e, n, depth)
            ups, downs = row_terms(h, e, n, depth)
            whole(main.at[t], a2a_r.at[0, t])
            whole(halo.at[t], a2a_r.at[1, t])
            new = []
            for f in range(3):
                window = jnp.concatenate([main[t, f], unpack(halo[t, f // per], f)], axis=1)
                value = window + cur[f] + DT * (rates[f] + shift_up(ups[f]) + shift_down(downs[f]))
                for yo in range(SP):
                    cs[t * SP + yo, f] = value[yo * RL : (yo + 1) * RL, :W]
                new.append(value)

            @pl.when(jnp.logical_and(t > 0, block == NG - 1))
            def _():
                give(t - 1)

            return tuple(new)

        @pl.when(block == 0)
        def _():
            cin[...] = jnp.zeros_like(cin)
            chalo[...] = jnp.zeros_like(chalo)

        @pl.when(block > 0)
        def _():
            for copy in carry():
                copy.wait_recv()
            give_begin(0, cin)

        first_state = tuple(
            jnp.concatenate(
                [jnp.concatenate([cin[yo, f] for yo in range(SP)], axis=0), unpack(chalo[f // per], f)], axis=1
            )
            for f in range(3)
        )
        last = lax.fori_loop(0, TG, turn, first_state)

        @pl.when(block == NG - 1)
        def _():
            give(TG - 1)

        @pl.when(block < NG - 1)
        def _():
            lanes = lax.broadcasted_iota(jnp.int32, (SP * RL, LANES), 1)
            slots = lax.rem(lanes + hw, LANES) // (2 * hw)
            for i in range(nh):
                packed = jnp.zeros((SP * RL, LANES), jnp.float32)
                for f in range(i * per, min(3, (i + 1) * per)):
                    z = last[f][:, W:]
                    if f % per:
                        z = pltpu.roll(z, 2 * hw * (f % per), 1)
                    packed = jnp.where(slots == f % per, z, packed)
                chalo_src[i] = packed
            for copy in carry():
                copy.start()

            @pl.loop(0, TG)
            def _(t):
                give(t)

    width = NX // GROUPS

    def fwd(q):
        cols = pl.ds(q * width, width)
        return pltpu.make_async_remote_copy(
            src_ref=ce.at[:, :, cols], dst_ref=cb.at[:, :, cols],
            send_sem=fwd_s.at[q], recv_sem=fwd_r.at[q], device_id=(lax.rem(p + 1, T), y), device_id_type=MESH,
        )

    for q in range(GROUPS):
        whole(ce.at[:, :, pl.ds(q * width, width)], ret_r.at[q])

        @pl.when(even)
        def _():
            fwd(q).start()

    @pl.when(p == 0)
    def _():
        cb[...] = init_ref[...]

    @pl.when(jnp.logical_and(even, p > 0))
    def _():
        whole(cb, beg_r)

    for q in range(GROUPS):
        @pl.when(jnp.logical_not(even))
        def _():
            fwd(q).wait_recv()

        cols = pl.ds(q * width, width)
        for f in range(3):
            start, end = cb[f, :, cols], ce[f, :, cols]
            out_ref[0, 0, f, :, cols] = start
            out_ref[0, 1, f, :, cols] = mid[f, :, cols] + 0.5 * (start + end)
            out_ref[0, 2, f, :, cols] = end

    @pl.when(p < T - 1)
    def _():
        shift.wait_send()

    @pl.when(even)
    def _():
        for q in range(GROUPS):
            fwd(q).wait_send()

    for stage in range(3):
        for side in range(2):
            edge_copy(stage, side).wait_send()
    for yo in range(SP):
        flat = pb * SP + yo

        @pl.when(jnp.logical_and(lax.rem(flat, stride) == 0, yo != y))
        def _():
            dep_copy(yo).wait_send()

    @pl.when(is_owner)
    def _():
        whole(b.at[:, :, pl.ds(0, (K - 1) * W)], a2a_s.at[0])
        whole(halo_src.at[:, :, pl.ds(0, (K - 1) * LANES)], a2a_s.at[1])
        whole(cs.at[pl.ds(0, TG * SP - 1)], ret_s)

        @pl.when(block < NG - 1)
        def _():
            for copy in carry():
                copy.wait_send()

        for t in range(0, TG, 2):
            for yo in range(SP):
                sent = jnp.logical_not(jnp.logical_and(t == pb, y == yo))
                if t == 0:
                    sent = jnp.logical_and(sent, block > 0)

                @pl.when(sent)
                def _():
                    pltpu.make_async_copy(cin.at[yo], cin.at[yo], beg_s.at[t * SP + yo]).wait()

    @pl.when(jnp.logical_not(is_owner))
    def _():
        whole(b, a2a_s.at[0])
        whole(halo_src, a2a_s.at[1])


def solution(mesh):
    T, SP = mesh.shape["tm"], mesh.shape["space"]

    def per_device(fine_nodes, init_state, mean_depth):
        RL, NX = mean_depth.shape
        NG = 2 if T % 4 == 0 else 1
        members = T // NG * SP
        W = max(LANES, NX // members)
        K = NX // W
        stride = members // K
        hw = 8
        while hw < T:
            hw *= 2
        per = LANES // (2 * hw)
        nh = -(-3 // per)
        cfg = (T, SP, RL, NX, W, K, stride, hw, per, nh, NG)
        f32, dma = jnp.float32, pltpu.SemaphoreType.DMA
        state = pltpu.VMEM((3, RL, NX), f32)
        R = RL * SP
        vmem = pl.BlockSpec(memory_space=pltpu.VMEM)
        return pl.pallas_call(
            functools.partial(kernel, cfg),
            out_shape=pltpu.VMEM(fine_nodes.shape, f32),
            in_specs=[pl.BlockSpec(memory_space=pl.ANY)] * 3,
            out_specs=vmem,
            scratch_shapes=[
                pltpu.VMEM((3, 3, RL, NX), f32), state, pltpu.VMEM((RL, NX), f32),
                state, state, state, state, state,
                pltpu.VMEM((nh, RL, K * LANES), f32),
                pltpu.VMEM((SP, RL, W + LANES), f32),
                pltpu.VMEM((R, W + LANES), f32),
                pltpu.VMEM((T // NG, 3, R, W), f32),
                pltpu.VMEM((T // NG, nh, R, LANES), f32),
                pltpu.VMEM((members, 3, RL, W), f32),
                state, state,
                pltpu.VMEM((3, 2, 3, 1, NX), f32),
                pltpu.VMEM((3, 2, 3, 1, NX), f32),
                pltpu.VMEM((SP, 3, RL, W), f32),
                pltpu.VMEM((nh, R, LANES), f32),
                pltpu.VMEM((nh, R, LANES), f32),
                dma, dma, dma((3, 2)), dma((3, 2)), dma((SP,)), dma, dma((2,)), dma((2, T // NG)),
                dma, dma((GROUPS,)), dma((GROUPS,)), dma((GROUPS,)),
                dma((2,)), dma((2,)), dma((members,)), dma, dma((5,)),
            ],
            compiler_params=pltpu.CompilerParams(
                collective_id=0, has_side_effects=True, vmem_limit_bytes=60 * 1024 * 1024
            ),
        )(fine_nodes, init_state, mean_depth)

    return jax.shard_map(
        per_device,
        mesh=mesh,
        in_specs=(P("tm", None, None, "space", None), P(None, "space", None), P("space", None)),
        out_specs=P("tm", None, None, "space", None),
        check_vma=False,
    )
```

```python
import functools

import jax
import jax.numpy as jnp
from jax import lax
from jax.experimental import pallas as pl
from jax.experimental.pallas import tpu as pltpu
from jax.sharding import PartitionSpec as P

MESH = pl.DeviceIdType.MESH
DT = 0.3
NU = 1.0 / 3.0
FC = 0.5
LANES = 128
GROUPS = 4


def shift_left(v):
    return pltpu.roll(v, v.shape[1] - 1, 1)


def shift_right(v):
    return pltpu.roll(v, 1, 1)


def shift_up(v):
    return pltpu.roll(v, v.shape[0] - 1, 0)


def shift_down(v):
    return pltpu.roll(v, 1, 0)


def row_terms(h, e, n, depth):
    dn = 0.5 * (depth * n)
    nh, ne, nn, hh = NU * h, NU * e, NU * n, 0.5 * h
    return (nh - dn, ne, nn - hh), (nh + dn, ne, nn + hh)


def column_terms(h, e, n, depth):
    de = 0.5 * (depth * e)
    nh, ne, nn, hh = NU * h, NU * e, NU * n, 0.5 * h
    return (
        shift_left(nh - de) + shift_right(nh + de) - 4.0 * nh,
        shift_left(ne - hh) + shift_right(ne + hh) - 4.0 * ne + FC * n,
        shift_left(nn) + shift_right(nn) - 4.0 * nn - FC * e,
    )


def kernel(
    cfg, u_hbm, init_hbm, depth_hbm, out_ref, u_ref, init_ref, depth_ref,
    s0, g, s1, mid, b, halo_src, dsrc, dep, main, halo, cs, ce, cb, esrc, edst, cin, chalo, chalo_src,
    shift_s, shift_r, edge_s, edge_r, dep_s, dep_r, a2a_s, a2a_r, ret_s, ret_r, fwd_s, fwd_r,
    c_s, c_r, beg_s, beg_r, in_s,
):
    T, SP, RL, NX, W, K, stride, hw, per, nh, NG = cfg
    TG = T // NG
    p, y = lax.axis_index("tm"), lax.axis_index("space")
    me = p * SP + y
    total = T * SP
    block = p // TG
    pb = p - block * TG
    local = pb * SP + y
    mine = local // stride
    is_owner = lax.rem(local, stride) == 0
    even = lax.rem(p, 2) == 0

    def where(flat):
        return (flat // SP, lax.rem(flat, SP))

    barrier = pltpu.get_barrier_semaphore()

    @pl.loop(1, total)
    def _(i):
        pl.semaphore_signal(barrier, inc=1, device_id=where(lax.rem(me + i, total)), device_id_type=MESH)

    loads = [pltpu.make_async_copy(u_hbm.at[0, i], u_ref.at[i], in_s.at[i]) for i in (2, 0, 1)]
    loads.append(pltpu.make_async_copy(depth_hbm, depth_ref, in_s.at[3]))
    loads.append(pltpu.make_async_copy(init_hbm, init_ref, in_s.at[4]))
    for copy in loads:
        copy.start()
    loads[0].wait()
    pl.semaphore_wait(barrier, total - 1)

    shift = pltpu.make_async_remote_copy(
        src_ref=u_ref.at[2], dst_ref=s0, send_sem=shift_s, recv_sem=shift_r,
        device_id=(lax.rem(p + 1, T), y), device_id_type=MESH,
    )

    @pl.when(p < T - 1)
    def _():
        shift.start()

    for copy in loads[1:]:
        copy.wait()

    lane_h = lax.broadcasted_iota(jnp.int32, (RL, LANES), 1)

    def dep_copy(yo):
        return pltpu.make_async_remote_copy(
            src_ref=dsrc.at[yo], dst_ref=dep.at[pl.ds(pl.multiple_of(y * RL, 8), RL)],
            send_sem=dep_s.at[yo], recv_sem=dep_r, device_id=(p, yo), device_id_type=MESH,
        )

    for yo in range(SP):
        flat = pb * SP + yo
        k = flat // stride

        @pl.when(lax.rem(flat, stride) == 0)
        def _():
            here = depth_ref[:, pl.ds(pl.multiple_of(k * W, LANES), W)]
            after = depth_ref[:, pl.ds(pl.multiple_of(lax.rem((k + 1) * W, NX), LANES), LANES)]
            before = depth_ref[:, pl.ds(pl.multiple_of(lax.rem(k * W + NX - LANES, NX), LANES), LANES)]
            dsrc[yo, :, :W] = here
            dsrc[yo, :, W:] = jnp.where(lane_h < LANES // 2, after, before)

            @pl.when(yo != y)
            def _():
                dep_copy(yo).start()

            @pl.when(yo == y)
            def _():
                pltpu.make_async_copy(
                    dsrc.at[yo], dep.at[pl.ds(pl.multiple_of(y * RL, 8), RL)], dep_r
                ).start()

    for f in range(3):
        g[f] = (-7.0 / 24.0) * u_ref[0, f] + (1.0 / 3.0) * u_ref[1, f] - (1.0 / 24.0) * u_ref[2, f]

    @pl.when(p > 0)
    def _():
        shift.wait_recv()

    @pl.when(p == 0)
    def _():
        s0[...] = init_ref[...]

    for f in range(3):
        g[f] = g[f] + 0.5 * s0[f]

    row = lax.broadcasted_iota(jnp.int32, (RL, NX), 0)

    def edge_copy(stage, side):
        to = lax.rem(y + SP - 1, SP) if side == 0 else lax.rem(y + 1, SP)
        return pltpu.make_async_remote_copy(
            src_ref=esrc.at[stage, side], dst_ref=edst.at[stage, side],
            send_sem=edge_s.at[stage, side], recv_sem=edge_r.at[stage, side],
            device_id=(p, to), device_id_type=MESH,
        )

    def rate_of_g(stage):
        up0, _ = row_terms(g[0, 0:1], g[1, 0:1], g[2, 0:1], depth_ref[0:1])
        _, down1 = row_terms(g[0, RL - 1 : RL], g[1, RL - 1 : RL], g[2, RL - 1 : RL], depth_ref[RL - 1 : RL])
        for f in range(3):
            esrc[stage, 0, f] = up0[f]
            esrc[stage, 1, f] = down1[f]
        for side in range(2):
            edge_copy(stage, side).start()
        h, e, n, depth = g[0], g[1], g[2], depth_ref[...]
        rates = column_terms(h, e, n, depth)
        ups, downs = row_terms(h, e, n, depth)
        for side in range(2):
            edge_copy(stage, side).wait_recv()
        return [
            rates[f]
            + jnp.where(row == RL - 1, edst[stage, 0, f], shift_up(ups[f]))
            + jnp.where(row == 0, edst[stage, 1, f], shift_down(downs[f]))
            for f in range(3)
        ]

    rates = rate_of_g(0)
    for f in range(3):
        s1[f] = s0[f] + DT * rates[f]
    for f in range(3):
        g[f] = (
            0.5 * s1[f]
            - (1.0 / 24.0) * u_ref[0, f] - (1.0 / 6.0) * u_ref[1, f] + (5.0 / 24.0) * u_ref[2, f]
        )
    rates = rate_of_g(1)
    first = jnp.where(p == 0, 1.0, 0.0).astype(jnp.float32)
    for f in range(3):
        s2 = s1[f] + DT * rates[f]
        g[f] = (1.0 / 6.0) * s2 + (2.0 / 3.0) * s1[f] + (first - 5.0 / 6.0) * s0[f]
        mid[f] = s1[f] - 0.5 * (s0[f] + s2)
    rates = rate_of_g(2)
    for f in range(3):
        b[f] = first * s0[f] + DT * rates[f]

    my_rows = pl.ds(pl.multiple_of(y * RL, 8), RL)

    def a2a(k):
        ends = (
            (b.at[:, :, pl.ds(pl.multiple_of(k * W, LANES), W)], main.at[pb, :, my_rows]),
            (halo_src.at[:, :, pl.ds(pl.multiple_of(k * LANES, LANES), LANES)], halo.at[pb, :, my_rows]),
        )
        there = [
            pltpu.make_async_remote_copy(
                src_ref=src, dst_ref=dst, send_sem=a2a_s.at[i], recv_sem=a2a_r.at[i, pb],
                device_id=where(block * TG * SP + k * stride), device_id_type=MESH,
            )
            for i, (src, dst) in enumerate(ends)
        ]
        here = [pltpu.make_async_copy(src, dst, a2a_r.at[i, pb]) for i, (src, dst) in enumerate(ends)]
        return there, here

    def spread(i):
        @pl.loop(0, K)
        def _(j):
            k = lax.rem(mine + j, K)
            there, here = a2a(k)

            @pl.when(k * stride != local)
            def _():
                there[i].start()

            @pl.when(k * stride == local)
            def _():
                here[i].start()

    spread(0)

    slot_of = lax.rem(lane_h + hw, LANES) // (2 * hw)
    for k in range(K):
        lo, hi = ((k + 1) % K) * W, (k * W - LANES) % NX
        packed = [jnp.zeros((RL, LANES), jnp.float32) for _ in range(nh)]
        for f in range(3):
            z = jnp.where(lane_h < LANES // 2, b[f, :, lo : lo + LANES], b[f, :, hi : hi + LANES])
            slot = f % per
            if slot:
                z = pltpu.roll(z, 2 * hw * slot, 1)
            packed[f // per] = jnp.where(slot_of == slot, z, packed[f // per])
        for i in range(nh):
            halo_src[i, :, k * LANES : (k + 1) * LANES] = packed[i]

    spread(1)

    my_tile = pl.ds(pl.multiple_of(mine * W, LANES), W)
    my_group = mine // (K // GROUPS)

    def give_back(t):
        for yo in range(SP):
            src, dst = cs.at[t * SP + yo], ce.at[:, :, my_tile]
            here = jnp.logical_and(t == pb, y == yo)

            @pl.when(jnp.logical_not(here))
            def _():
                pltpu.make_async_remote_copy(
                    src_ref=src, dst_ref=dst, send_sem=ret_s, recv_sem=ret_r.at[my_group],
                    device_id=(block * TG + t, yo), device_id_type=MESH,
                ).start()

            @pl.when(here)
            def _():
                pltpu.make_async_copy(src, dst, ret_r.at[my_group]).start()

    def give_begin(t, src):
        for yo in range(SP):
            dst = cb.at[:, :, my_tile]
            here = jnp.logical_and(t == pb, y == yo)

            @pl.when(jnp.logical_not(here))
            def _():
                pltpu.make_async_remote_copy(
                    src_ref=src.at[yo], dst_ref=dst, send_sem=beg_s.at[t * SP + yo], recv_sem=beg_r,
                    device_id=(block * TG + t, yo), device_id_type=MESH,
                ).start()

            @pl.when(here)
            def _():
                pltpu.make_async_copy(src.at[yo], dst, beg_r).start()

    def give(t):
        give_back(t)

        @pl.when(jnp.logical_and(lax.rem(t, 2) == 1, t < TG - 1))
        def _():
            give_begin(t + 1, cs.at[pl.ds(t * SP, SP)])

    def carry():
        ends = ((cs.at[pl.ds((TG - 1) * SP, SP)], cin), (chalo_src, chalo))
        return [
            pltpu.make_async_remote_copy(
                src_ref=src, dst_ref=dst, send_sem=c_s.at[i], recv_sem=c_r.at[i],
                device_id=(lax.rem(p + TG, T), y), device_id_type=MESH,
            )
            for i, (src, dst) in enumerate(ends)
        ]

    def unpack(tile, f):
        return pltpu.roll(tile, LANES - 2 * hw * (f % per), 1) if f % per else tile

    def whole(ref, sem):
        pltpu.make_async_copy(ref, ref, sem).wait()

    @pl.when(is_owner)
    def _():
        whole(dep, dep_r)
        depth = dep[...]

        def turn(t, cur):
            h, e, n = cur
            rates = column_terms(h, e, n, depth)
            ups, downs = row_terms(h, e, n, depth)
            whole(main.at[t], a2a_r.at[0, t])
            whole(halo.at[t], a2a_r.at[1, t])
            new = []
            for f in range(3):
                window = jnp.concatenate([main[t, f], unpack(halo[t, f // per], f)], axis=1)
                value = window + cur[f] + DT * (rates[f] + shift_up(ups[f]) + shift_down(downs[f]))
                for yo in range(SP):
                    cs[t * SP + yo, f] = value[yo * RL : (yo + 1) * RL, :W]
                new.append(value)

            @pl.when(jnp.logical_and(t > 0, block == NG - 1))
            def _():
                give(t - 1)

            return tuple(new)

        @pl.when(block == 0)
        def _():
            cin[...] = jnp.zeros_like(cin)
            chalo[...] = jnp.zeros_like(chalo)

        @pl.when(block > 0)
        def _():
            for copy in carry():
                copy.wait_recv()
            give_begin(0, cin)

        first_state = tuple(
            jnp.concatenate(
                [jnp.concatenate([cin[yo, f] for yo in range(SP)], axis=0), unpack(chalo[f // per], f)], axis=1
            )
            for f in range(3)
        )
        last = lax.fori_loop(0, TG, turn, first_state)

        @pl.when(block == NG - 1)
        def _():
            give(TG - 1)

        @pl.when(block < NG - 1)
        def _():
            lanes = lax.broadcasted_iota(jnp.int32, (SP * RL, LANES), 1)
            slots = lax.rem(lanes + hw, LANES) // (2 * hw)
            for i in range(nh):
                packed = jnp.zeros((SP * RL, LANES), jnp.float32)
                for f in range(i * per, min(3, (i + 1) * per)):
                    z = last[f][:, W:]
                    if f % per:
                        z = pltpu.roll(z, 2 * hw * (f % per), 1)
                    packed = jnp.where(slots == f % per, z, packed)
                chalo_src[i] = packed
            for copy in carry():
                copy.start()

            @pl.loop(0, TG)
            def _(t):
                give(t)

    width = NX // GROUPS

    def fwd(q):
        cols = pl.ds(q * width, width)
        return pltpu.make_async_remote_copy(
            src_ref=ce.at[:, :, cols], dst_ref=cb.at[:, :, cols],
            send_sem=fwd_s.at[q], recv_sem=fwd_r.at[q], device_id=(lax.rem(p + 1, T), y), device_id_type=MESH,
        )

    for q in range(GROUPS):
        whole(ce.at[:, :, pl.ds(q * width, width)], ret_r.at[q])

        @pl.when(even)
        def _():
            fwd(q).start()

    @pl.when(p == 0)
    def _():
        cb[...] = init_ref[...]

    @pl.when(jnp.logical_and(even, p > 0))
    def _():
        whole(cb, beg_r)

    for q in range(GROUPS):
        @pl.when(jnp.logical_not(even))
        def _():
            fwd(q).wait_recv()

        cols = pl.ds(q * width, width)
        for f in range(3):
            start, end = cb[f, :, cols], ce[f, :, cols]
            out_ref[0, 0, f, :, cols] = start
            out_ref[0, 1, f, :, cols] = mid[f, :, cols] + 0.5 * (start + end)
            out_ref[0, 2, f, :, cols] = end

    @pl.when(p < T - 1)
    def _():
        shift.wait_send()

    @pl.when(even)
    def _():
        for q in range(GROUPS):
            fwd(q).wait_send()

    for stage in range(3):
        for side in range(2):
            edge_copy(stage, side).wait_send()
    for yo in range(SP):
        flat = pb * SP + yo

        @pl.when(jnp.logical_and(lax.rem(flat, stride) == 0, yo != y))
        def _():
            dep_copy(yo).wait_send()

    @pl.when(is_owner)
    def _():
        whole(b.at[:, :, pl.ds(0, (K - 1) * W)], a2a_s.at[0])
        whole(halo_src.at[:, :, pl.ds(0, (K - 1) * LANES)], a2a_s.at[1])
        whole(cs.at[pl.ds(0, TG * SP - 1)], ret_s)

        @pl.when(block < NG - 1)
        def _():
            for copy in carry():
                copy.wait_send()

        for t in range(0, TG, 2):
            for yo in range(SP):
                sent = jnp.logical_not(jnp.logical_and(t == pb, y == yo))
                if t == 0:
                    sent = jnp.logical_and(sent, block > 0)

                @pl.when(sent)
                def _():
                    pltpu.make_async_copy(cin.at[yo], cin.at[yo], beg_s.at[t * SP + yo]).wait()

    @pl.when(jnp.logical_not(is_owner))
    def _():
        whole(b, a2a_s.at[0])
        whole(halo_src, a2a_s.at[1])


def solution(mesh):
    T, SP = mesh.shape["tm"], mesh.shape["space"]

    def per_device(fine_nodes, init_state, mean_depth):
        RL, NX = mean_depth.shape
        NG = 2 if T % 4 == 0 else 1
        members = T // NG * SP
        W = max(LANES, NX // members)
        K = NX // W
        stride = members // K
        hw = 8
        while hw < T:
            hw *= 2
        per = LANES // (2 * hw)
        nh = -(-3 // per)
        cfg = (T, SP, RL, NX, W, K, stride, hw, per, nh, NG)
        f32, dma = jnp.float32, pltpu.SemaphoreType.DMA
        state = pltpu.VMEM((3, RL, NX), f32)
        R = RL * SP
        vmem = pl.BlockSpec(memory_space=pltpu.VMEM)
        return pl.pallas_call(
            functools.partial(kernel, cfg),
            out_shape=pltpu.VMEM(fine_nodes.shape, f32),
            in_specs=[pl.BlockSpec(memory_space=pl.ANY)] * 3,
            out_specs=vmem,
            scratch_shapes=[
                pltpu.VMEM((3, 3, RL, NX), f32), state, pltpu.VMEM((RL, NX), f32),
                state, state, state, state, state,
                pltpu.VMEM((nh, RL, K * LANES), f32),
                pltpu.VMEM((SP, RL, W + LANES), f32),
                pltpu.VMEM((R, W + LANES), f32),
                pltpu.VMEM((T // NG, 3, R, W), f32),
                pltpu.VMEM((T // NG, nh, R, LANES), f32),
                pltpu.VMEM((members, 3, RL, W), f32),
                state, state,
                pltpu.VMEM((3, 2, 3, 1, NX), f32),
                pltpu.VMEM((3, 2, 3, 1, NX), f32),
                pltpu.VMEM((SP, 3, RL, W), f32),
                pltpu.VMEM((nh, R, LANES), f32),
                pltpu.VMEM((nh, R, LANES), f32),
                dma, dma, dma((3, 2)), dma((3, 2)), dma((SP,)), dma, dma((2,)), dma((2, T // NG)),
                dma, dma((GROUPS,)), dma((GROUPS,)), dma((GROUPS,)),
                dma((2,)), dma((2,)), dma((members,)), dma, dma((5,)),
            ],
            compiler_params=pltpu.CompilerParams(
                collective_id=0, has_side_effects=True, vmem_limit_bytes=60 * 1024 * 1024
            ),
        )(fine_nodes, init_state, mean_depth)

    return jax.shard_map(
        per_device,
        mesh=mesh,
        in_specs=(P("tm", None, None, "space", None), P(None, "space", None), P("space", None)),
        out_specs=P("tm", None, None, "space", None),
        check_vma=False,
    )
```
